32 devices in a mesh: cls: 8 (over z, y), row: 4 (over x, core).
Axes of the slice: x: 2, y: 2, z: 4, core: 2. Of those that a mesh axis runs over, the one named last changes fastest.
Arguments:
- embeddings: float32 [1024, 1024], P('row'), may hold values from -6 to 6
- weights: float32 [1024, 81920], P(('cls', 'row')), may hold values from -4 to 4
- labels: int32 [1024], replicated, may hold values from 0 to 81919, as said below
Outputs:
- weight_update: float32 [1024, 81920], P(None, ('cls', 'row'))
- losses: float32 [2, 1024], replicated
The draws below stay inside these ranges and needn't reach their ends.
Inputs may be any that keep to these rules, and one draw needn't show every extreme that they name: labels take at most 512 distinct values, at most one in each aligned run of 160 classes; rows may share a label.
All inputs are finite; a program needn't handle non-finite values.
Results may differ from the reference program's by a relative error of at most 0.012.
The reference program's roundings to bfloat16 on the way count: a program that leaves them out, or rounds other values in their place, can miss the bound.
Values may be sent and summed in bfloat16 or wider, within the bound.
A program may use at most 128 MiB of HBM per device.

```python
import math
import jax
import jax.numpy as jnp
from jax import lax

D = 1024
CLS_DEV = 2560
STEPS = 2
ROWS = 1024
CLASSES = 81920


def embedding_draw(key):
    noise = jax.random.normal(jax.random.fold_in(key, 7), (ROWS, D), jnp.float32)
    return jnp.clip(noise + 0.5, -6.0, 6.0)


def draw_embeddings(key, part):
    return embedding_draw(key)


def draw_weights(key, part):
    base = jax.random.normal(jax.random.fold_in(key, 9), (D, CLASSES), jnp.float32) * (8.0 / math.sqrt(D))
    base = jnp.clip(base, -4.0, 4.0)
    return base


def draw_labels(key, part):
    run_width = CLASSES // 512
    slots = jax.random.randint(jax.random.fold_in(key, 21), (ROWS,), 0, 512, dtype=jnp.int32)
    slots = slots.at[0].set(0).at[ROWS - 1].set(511)
    offsets = jax.random.randint(jax.random.fold_in(key, 22), (512,), 0, run_width, dtype=jnp.int32)
    offsets = offsets.at[0].set(0).at[511].set(run_width - 1)
    return (slots * run_width + offsets[slots]).astype(jnp.int32)


def setup_inputs(seed: int = 0) -> dict:
    arg_keys = jax.random.split(jax.random.key(seed), 4)
    return {
        "embeddings": draw_embeddings(jax.random.fold_in(arg_keys[3], 71), 0),
        "weights": draw_weights(jax.random.fold_in(arg_keys[3], 71), 0),
        "labels": draw_labels(jax.random.fold_in(arg_keys[3], 71), 0),
    }


learn_rate = 2.0


def reference(embeddings, weights, labels):
    rounded = embeddings.astype(jnp.bfloat16)
    row_count = rounded.shape[0]
    block_count = CLASSES // CLS_DEV
    columns = jnp.arange(CLS_DEV, dtype=jnp.int32)
    starts = jnp.arange(block_count, dtype=jnp.int32) * CLS_DEV
    current = weights
    loss_rows = []
    for step_index in range(STEPS):
        stacked = current.reshape(D, block_count, CLS_DEV).transpose(1, 0, 2)

        def block_stats(operands):
            class_block, start = operands
            logits = jnp.dot(rounded, class_block.astype(jnp.bfloat16), preferred_element_type=jnp.float32)
            block_peak = jnp.max(logits, axis=1)
            block_total = jnp.sum(jnp.exp(logits - block_peak[:, None]), axis=1)
            label_hit = (columns[None, :] + start) == labels[:, None]
            block_picked = jnp.sum(jnp.where(label_hit, logits, jnp.float32(0.0)), axis=1)
            return block_peak, block_total, block_picked

        peaks, totals, pickeds = lax.map(block_stats, (stacked, starts))
        row_peak = jnp.max(peaks, axis=0)
        row_total = jnp.sum(totals * jnp.exp(peaks - row_peak[None, :]), axis=0)
        picked = jnp.sum(pickeds, axis=0)
        log_norm = row_peak + jnp.log(row_total)
        loss_rows.append(log_norm - picked)

        def block_update(operands):
            class_block, start = operands
            logits = jnp.dot(rounded, class_block.astype(jnp.bfloat16), preferred_element_type=jnp.float32)
            label_hit = (columns[None, :] + start) == labels[:, None]
            onehot = jnp.where(label_hit, jnp.float32(1.0), jnp.float32(0.0))
            residual = (jnp.exp(logits - log_norm[:, None]) - onehot).astype(jnp.bfloat16)
            gradient = jnp.dot(rounded.T, residual, preferred_element_type=jnp.float32) / row_count
            return class_block - learn_rate * gradient

        renewed = lax.map(block_update, (stacked, starts))
        current = renewed.transpose(1, 0, 2).reshape(D, CLASSES)
    return current - weights, jnp.stack(loss_rows)
```

```python
import functools

import jax
import jax.numpy as jnp
from jax import lax
from jax.experimental import pallas as pl
from jax.experimental.pallas import tpu as pltpu
from jax.sharding import PartitionSpec as P

STEPS = 2


learn_rate = 2.0

MESH = pl.DeviceIdType.MESH
LANES = 128
ROW_TILE = 256
SUB = 32
HALVES = 2
LOG2E = 1.4426950408889634
LN2 = 0.6931471805599453
KERNEL_VMEM = 40 * 1024 * 1024
UPDATE_VMEM = 24 * 1024 * 1024


def exchange_kernel(
    cls_n,
    row_n,
    rate,
    emb_hbm,
    weights_ref,
    labels_hbm,
    total_ref,
    turned_ref,
    losses_ref,
    stage,
    outgoing,
    incoming,
    label_lanes,
    logits,
    gram,
    examples,
    emb_ref,
    emb_bf,
    labels_ref,
    peak_lanes,
    sum_lanes,
    pick_lanes,
    norm_lanes,
    hit_lanes,
    first_send,
    first_recv,
    later_send,
    later_recv,
    load_sem,
    small_sem,
    out_sem,
    in_sem,
    emb_out,
    emb_in,
    first_out,
    first_in,
    later_out,
    later_in,
):
    n = cls_n * row_n
    my_cls, my_row = lax.axis_index("cls"), lax.axis_index("row")
    me = my_cls * row_n + my_row
    chunks, rows, width = logits.shape
    pieces, _, features, narrow = outgoing.shape
    per = width // narrow
    class_count = chunks * width
    shard_rows = emb_ref.shape[0]
    tiles = rows // ROW_TILE
    groups = width // LANES
    slabs = rows // LANES

    def place(p):
        return (lax.div(p, row_n), lax.rem(p, row_n))

    barrier = pltpu.get_barrier_semaphore()

    @pl.loop(1, n)
    def _(k):
        pl.semaphore_signal(
            barrier, inc=1, device_id=place(lax.rem(me + k, n)), device_id_type=MESH
        )

    def load(piece, slot):
        @pl.loop(0, n)
        def _(p):
            start = pl.multiple_of(p * class_count + piece * narrow, LANES)
            pltpu.make_async_copy(
                weights_ref.at[:, pl.ds(start, narrow)], stage.at[slot, p], load_sem.at[slot]
            ).start()

    load(0, 0)
    emb_copy = pltpu.make_async_copy(emb_hbm, emb_ref, small_sem.at[0])
    emb_copy.start()
    labels_copy = pltpu.make_async_copy(labels_hbm, labels_ref, small_sem.at[1])
    labels_copy.start()
    load(1, 1)

    emb_copy.wait()
    emb_bf[...] = emb_ref[...].astype(jnp.bfloat16)
    mine = pl.ds(pl.multiple_of(my_row * shard_rows, shard_rows), shard_rows)
    examples[mine, :] = emb_bf[...]
    labels_copy.wait()
    pl.semaphore_wait(barrier, n - 1)

    @pl.loop(0, pieces)
    def _(c):
        slot = lax.rem(c, 2)
        pltpu.make_async_copy(stage.at[slot], stage.at[slot], load_sem.at[slot]).wait()
        spot = pl.ds(pl.multiple_of(me * features, features), features)

        def send(j):
            p = lax.rem(me + j + n // 2, n)
            outgoing[c, p] = stage[slot, p].astype(jnp.bfloat16)
            pltpu.make_async_remote_copy(
                src_ref=outgoing.at[c, p],
                dst_ref=incoming.at[c, spot],
                send_sem=out_sem.at[c],
                recv_sem=in_sem.at[c],
                device_id=place(p),
                device_id_type=MESH,
            ).start()

        pl.loop(0, n // 2)(send)
        incoming[c, spot] = stage[slot, me].astype(jnp.bfloat16)
        pl.loop(n // 2 + 1, n)(send)

        @pl.when(c == 0)
        def _():
            @pl.loop(1, row_n)
            def _(k):
                pltpu.make_async_remote_copy(
                    src_ref=emb_bf,
                    dst_ref=examples.at[mine],
                    send_sem=emb_out,
                    recv_sem=emb_in,
                    device_id=(my_cls, lax.rem(my_row + k, row_n)),
                    device_id_type=MESH,
                ).start()

        @pl.when(c + 2 < pieces)
        def _():
            load(c + 2, slot)

    for i in range(slabs):
        label_lanes[pl.ds(i * LANES, LANES), :] = (
            jnp.broadcast_to(labels_ref[i : i + 1, :], (LANES, LANES)).T - me * class_count
        )

    peers = pl.ds(0, (row_n - 1) * shard_rows)
    pltpu.make_async_copy(examples.at[peers], examples.at[peers], emb_in).wait()

    @pl.loop(0, tiles)
    def _(i):
        here = pl.ds(pl.multiple_of(i * ROW_TILE, ROW_TILE), ROW_TILE)
        product = lax.dot_general(
            examples[here, :],
            examples[...],
            (((1,), (1,)), ((), ())),
            preferred_element_type=jnp.float32,
        )
        gram[here, :] = (product * (rate * LOG2E)).astype(jnp.bfloat16)
        turned_ref[:, here] = examples[here, :].astype(jnp.float32).T.astype(jnp.bfloat16)

    def reset():
        peak_lanes[...] = jnp.full_like(peak_lanes, -3.0e38)
        sum_lanes[...] = jnp.zeros_like(sum_lanes)
        pick_lanes[...] = jnp.zeros_like(pick_lanes)

    def hits(spot, offset, count):
        shifted = label_lanes[spot, :] - offset
        lane = lax.broadcasted_iota(jnp.int32, shifted.shape, 1)
        return [lane + q * LANES == shifted for q in range(count)]

    def collect(spot, offset, block):
        count = block.shape[1] // LANES
        parts = [block[:, q * LANES : (q + 1) * LANES] for q in range(count)]
        old = peak_lanes[spot, :]
        peak = functools.reduce(jnp.maximum, parts, old)
        total = sum_lanes[spot, :] * jnp.exp2(old - peak)
        picked = pick_lanes[spot, :]
        for part, hit in zip(parts, hits(spot, offset, count)):
            total = total + jnp.exp2(part - peak)
            picked = jnp.where(hit, part, picked)
        peak_lanes[spot, :] = peak
        sum_lanes[spot, :] = total
        pick_lanes[spot, :] = picked

    def residual(c, spot, earlier):
        norm = norm_lanes[spot, :]
        at_label = hit_lanes[spot, :]
        for q, hit in enumerate(hits(spot, c * width, groups)):
            columns = slice(q * LANES, (q + 1) * LANES)
            part = logits[c, spot, columns]
            value = jnp.where(hit, at_label, jnp.exp2(part - norm)).astype(jnp.bfloat16)
            if earlier:
                value = value + total_ref[c, spot, columns]
            total_ref[c, spot, columns] = value

    def share(src, dst, send_sem, recv_sem):
        @pl.loop(1, n)
        def _(k):
            pltpu.make_async_remote_copy(
                src_ref=src,
                dst_ref=dst.at[me],
                send_sem=send_sem,
                recv_sem=recv_sem,
                device_id=place(lax.rem(me + k, n)),
                device_id_type=MESH,
            ).start()

    def publish(first, count, sent, landed, send_sem, recv_sem):
        for i in range(count):
            part = pl.ds((first + i) * LANES, LANES)
            peaks = peak_lanes[part, :].T
            top = jnp.max(peaks, axis=0, keepdims=True)
            total = jnp.sum(sum_lanes[part, :].T * jnp.exp2(peaks - top), axis=0, keepdims=True)
            sent[0, i : i + 1, :] = top + jnp.log(total) * LOG2E
        landed[0, me] = sent[0]
        share(sent.at[0], landed.at[0], send_sem.at[0], recv_sem.at[0])
        for i in range(count):
            part = pl.ds((first + i) * LANES, LANES)
            sent[1, i : i + 1, :] = jnp.sum(pick_lanes[part, :].T, axis=0, keepdims=True)
        landed[1, me] = sent[1]
        share(sent.at[1], landed.at[1], send_sem.at[1], recv_sem.at[1])

    others = pl.ds(0, n - 1)

    def agree(first, count, sent, landed, recv_sem):
        arrived = landed.at[0, others]
        pltpu.make_async_copy(arrived, arrived, recv_sem.at[0]).wait()
        norms = landed[0]
        top = jnp.max(norms, axis=0)
        norm = top + jnp.log(jnp.sum(jnp.exp2(norms - top[None]), axis=0)) * LOG2E
        at_label = jnp.exp2(sent[1] - norm) - 1.0
        for i in range(count):
            part = pl.ds((first + i) * LANES, LANES)
            norm_lanes[part, :] = jnp.broadcast_to(norm[i : i + 1, :], (LANES, LANES)).T
            hit_lanes[part, :] = jnp.broadcast_to(at_label[i : i + 1, :], (LANES, LANES)).T
        return norm

    def finish(step, first, count, norm, landed, send_sem, recv_sem):
        arrived = landed.at[1, others]
        pltpu.make_async_copy(arrived, arrived, recv_sem.at[1]).wait()
        loss = (norm - jnp.sum(landed[1], axis=0)) * LN2
        for i in range(count):
            columns = slice((first + i) * LANES, (first + i + 1) * LANES)
            losses_ref[step : step + 1, columns] = loss[i : i + 1, :]
        for kind in range(2):
            done = landed.at[kind, others]
            pltpu.make_async_copy(done, done, send_sem.at[kind]).wait()

    reset()

    @pl.loop(0, chunks)
    def _(c):
        for h in range(per):
            piece = c * per + h
            arrived = pl.ds(0, (n - 1) * features)
            pltpu.make_async_copy(
                incoming.at[piece, arrived], incoming.at[piece, arrived], in_sem.at[piece]
            ).wait()
            columns = slice(h * narrow, (h + 1) * narrow)

            @pl.loop(0, tiles)
            def _(i):
                here = pl.ds(pl.multiple_of(i * ROW_TILE, ROW_TILE), ROW_TILE)
                logits[c, here, columns] = (
                    jnp.dot(examples[here, :], incoming[piece], preferred_element_type=jnp.float32)
                    * LOG2E
                )

                @pl.loop(0, ROW_TILE // SUB, unroll=2)
                def _(u):
                    spot = pl.ds(pl.multiple_of(i * ROW_TILE + u * SUB, SUB), SUB)
                    collect(spot, piece * narrow, logits[c, spot, columns])

    publish(0, slabs, first_send, first_recv, first_out, first_in)
    first_norm = agree(0, slabs, first_send, first_recv, first_in)
    reset()

    @pl.loop(0, rows // SUB, unroll=4)
    def _(u):
        residual(0, pl.ds(pl.multiple_of(u * SUB, SUB), SUB), False)

    half = slabs // HALVES
    half_tiles = tiles // HALVES
    share_rows = rows // half_tiles
    for h in range(HALVES):
        for c in range(chunks):
            for i in range(half_tiles):
                here = pl.ds((h * half_tiles + i) * ROW_TILE, ROW_TILE)
                change = jnp.dot(gram[here, :], total_ref[c], preferred_element_type=jnp.float32)
                if h == 0 and c + 1 < chunks:
                    residual(c + 1, pl.ds(i * share_rows, share_rows), False)
                block = logits[c, here, :] - change
                logits[c, here, :] = block
                collect(here, c * width, block)
        publish(
            h * half, half, later_send.at[h], later_recv.at[h], later_out.at[h], later_in.at[h]
        )

    finish(0, 0, slabs, first_norm, first_recv, first_out, first_in)
    later_norms = []
    for h in range(HALVES):
        later_norms.append(agree(h * half, half, later_send.at[h], later_recv.at[h], later_in.at[h]))

        @pl.loop(0, rows // HALVES // SUB, unroll=2)
        def _(u):
            spot = pl.ds(pl.multiple_of(h * (rows // HALVES) + u * SUB, SUB), SUB)
            for c in range(chunks):
                residual(c, spot, True)

    for h in range(HALVES):
        finish(1, h * half, half, later_norms[h], later_recv.at[h], later_out.at[h], later_in.at[h])

    pltpu.make_async_copy(examples.at[peers], examples.at[peers], emb_out).wait()

    @pl.loop(0, pieces)
    def _(c):
        sent = pl.ds(0, n - 1)
        pltpu.make_async_copy(outgoing.at[c, sent], outgoing.at[c, sent], out_sem.at[c]).wait()


def update_kernel(rate, turned_ref, total_ref, losses_in, out_ref, losses_ref, held, out_sem):
    chunks, model_width, width = held.shape
    losses_ref[...] = losses_in[...]
    copies = []
    for c in range(chunks):
        for i in range(model_width // ROW_TILE):
            here = pl.ds(i * ROW_TILE, ROW_TILE)
            held[c, here, :] = -rate * jnp.dot(
                turned_ref[here, :], total_ref[c], preferred_element_type=jnp.float32
            )
            copies.append(
                pltpu.make_async_copy(
                    held.at[c, here],
                    out_ref.at[here, pl.ds(c * width, width)],
                    out_sem.at[c, i],
                )
            )
            copies[-1].start()
    for copy in copies:
        copy.wait()


def fused(embeddings, weights, labels):
    cls_n, row_n = lax.axis_size("cls"), lax.axis_size("row")
    n = cls_n * row_n
    shard_rows, model_width = embeddings.shape
    rows = shard_rows * row_n
    features = weights.shape[0]
    class_count = weights.shape[1] // n
    width = max(w for w in (128, 256, 384, 512) if class_count % w == 0)
    narrow = 256 if width % 256 == 0 else LANES
    chunks = class_count // width
    pieces = class_count // narrow
    rate = learn_rate / rows
    slabs = rows // LANES
    half = slabs // HALVES
    vmem = pl.BlockSpec(memory_space=pltpu.VMEM)
    hbm = pl.BlockSpec(memory_space=pltpu.HBM)
    dma = pltpu.SemaphoreType.DMA
    lanes = pltpu.VMEM((rows, LANES), jnp.float32)
    operands = (embeddings, weights, labels.reshape(slabs, LANES))
    total, turned, losses = pl.pallas_call(
        functools.partial(exchange_kernel, cls_n, row_n, rate),
        out_shape=(
            jax.ShapeDtypeStruct((chunks, rows, width), jnp.bfloat16),
            jax.ShapeDtypeStruct((model_width, rows), jnp.bfloat16),
            jax.ShapeDtypeStruct((STEPS, rows), jnp.float32),
        ),
        in_specs=[hbm, hbm, hbm],
        out_specs=(vmem, vmem, vmem),
        scratch_shapes=[
            pltpu.VMEM((2, n, features, narrow), jnp.float32),
            pltpu.VMEM((pieces, n, features, narrow), jnp.bfloat16),
            pltpu.VMEM((pieces, n * features, narrow), jnp.bfloat16),
            pltpu.VMEM((rows, LANES), jnp.int32),
            pltpu.VMEM((chunks, rows, width), jnp.float32),
            pltpu.VMEM((rows, rows), jnp.bfloat16),
            pltpu.VMEM((rows, model_width), jnp.bfloat16),
            pltpu.VMEM((shard_rows, model_width), jnp.float32),
            pltpu.VMEM((shard_rows, model_width), jnp.bfloat16),
            pltpu.VMEM((slabs, LANES), jnp.int32),
            lanes,
            lanes,
            lanes,
            lanes,
            lanes,
            pltpu.VMEM((2, slabs, LANES), jnp.float32),
            pltpu.VMEM((2, n, slabs, LANES), jnp.float32),
            pltpu.VMEM((HALVES, 2, half, LANES), jnp.float32),
            pltpu.VMEM((HALVES, 2, n, half, LANES), jnp.float32),
            dma((2,)),
            dma((2,)),
            dma((pieces,)),
            dma((pieces,)),
            dma,
            dma,
            dma((2,)),
            dma((2,)),
            dma((HALVES, 2)),
            dma((HALVES, 2)),
        ],
        compiler_params=pltpu.CompilerParams(
            collective_id=0, has_side_effects=True, vmem_limit_bytes=KERNEL_VMEM
        ),
    )(*(pltpu.with_memory_space_constraint(x, pltpu.HBM) for x in operands))
    update, losses = pl.pallas_call(
        functools.partial(update_kernel, rate),
        out_shape=(
            jax.ShapeDtypeStruct((model_width, class_count), jnp.float32),
            jax.ShapeDtypeStruct((STEPS, rows), jnp.float32),
        ),
        in_specs=[vmem, vmem, vmem],
        out_specs=(hbm, vmem),
        scratch_shapes=[
            pltpu.VMEM((chunks, model_width, width), jnp.float32),
            dma((chunks, model_width // ROW_TILE)),
        ],
        compiler_params=pltpu.CompilerParams(vmem_limit_bytes=UPDATE_VMEM),
    )(turned, total, losses)
    return update, losses


def shards(embeddings, weights, labels):
    if STEPS == 2 and weights.shape[0] % 16 == 0:
        return fused(embeddings, weights, labels)
    peer_count = lax.axis_size(("cls", "row"))
    examples = lax.all_gather(embeddings.astype(jnp.bfloat16), "row", axis=0, tiled=True)
    row_count = examples.shape[0]
    feature_rows = weights.shape[0]
    class_count = weights.shape[1] // peer_count
    offset = lax.axis_index(("cls", "row")) * class_count
    columns = lax.broadcasted_iota(jnp.int32, (1, class_count), 1) + offset
    label_hit = columns == labels[:, None]
    pieces = weights.astype(jnp.bfloat16).reshape(feature_rows, peer_count, class_count)
    block_weights = lax.all_to_all(
        pieces.transpose(1, 0, 2), ("cls", "row"), split_axis=0, concat_axis=0, tiled=True
    )
    flat_weights = block_weights.reshape(peer_count * feature_rows, class_count)
    first_logits = jnp.dot(examples, flat_weights, preferred_element_type=jnp.float32)
    rate = learn_rate / row_count
    gram = lax.dot_general(
        examples, examples, (((1,), (1,)), ((), ())), preferred_element_type=jnp.float32
    ).astype(jnp.bfloat16)
    total = None
    loss_rows = []
    for step_index in range(STEPS):
        logits = first_logits
        if step_index > 0:
            logits = logits - rate * jnp.dot(gram, total, preferred_element_type=jnp.float32)
        local_peak = jnp.max(logits, axis=1)
        local_total = jnp.sum(jnp.exp(logits - local_peak[:, None]), axis=1)
        local_picked = jnp.sum(jnp.where(label_hit, logits, 0.0), axis=1)
        stats = lax.all_gather(
            jnp.stack([local_peak, local_total, local_picked]), ("cls", "row"), axis=0
        )
        row_peak = jnp.max(stats[:, 0], axis=0)
        row_total = jnp.sum(stats[:, 1] * jnp.exp(stats[:, 0] - row_peak[None, :]), axis=0)
        picked = jnp.sum(stats[:, 2], axis=0)
        log_norm = row_peak + jnp.log(row_total)
        loss_rows.append(log_norm - picked)
        onehot = jnp.where(label_hit, 1.0, 0.0)
        residual = jnp.exp(logits - log_norm[:, None]) - onehot
        if total is not None:
            residual = residual + total.astype(jnp.float32)
        total = residual.astype(jnp.bfloat16)
    update = lax.dot_general(
        examples, total, (((0,), (0,)), ((), ())), preferred_element_type=jnp.float32
    )
    return (-rate * update, jnp.stack(loss_rows))


def solution(mesh):
    placed = (P("row", None), P(("cls", "row"), None), P())
    return jax.shard_map(
        shards,
        mesh=mesh,
        in_specs=placed,
        out_specs=(P(None, ("cls", "row")), P()),
        check_vma=False,
    )
```

```python
import functools

import jax
import jax.numpy as jnp
from jax import lax
from jax.experimental import pallas as pl
from jax.experimental.pallas import tpu as pltpu
from jax.sharding import PartitionSpec as P

STEPS = 2


learn_rate = 2.0

MESH = pl.DeviceIdType.MESH
LANES = 128
ROW_TILE = 256
SUB = 32
LOG2E = 1.4426950408889634
LN2 = 0.6931471805599453
KERNEL_VMEM = 40 * 1024 * 1024
UPDATE_VMEM = 24 * 1024 * 1024


def exchange_kernel(
    cls_n,
    row_n,
    rate,
    emb_hbm,
    weights_ref,
    labels_hbm,
    update_ref,
    late_ref,
    late_turned,
    losses_ref,
    stage,
    outgoing,
    incoming,
    label_lanes,
    logits,
    gram,
    examples,
    early_turned,
    emb_ref,
    emb_bf,
    labels_ref,
    peak_lanes,
    sum_lanes,
    pick_lanes,
    norm_lanes,
    hit_lanes,
    first_send,
    first_recv,
    later_send,
    later_recv,
    load_sem,
    small_sem,
    out_sem,
    in_sem,
    emb_out,
    emb_in,
    first_out,
    first_in,
    later_out,
    later_in,
):
    n = cls_n * row_n
    my_cls, my_row = lax.axis_index("cls"), lax.axis_index("row")
    me = my_cls * row_n + my_row
    chunks, rows, width = logits.shape
    pieces, _, features, narrow = outgoing.shape
    per = width // narrow
    class_count = chunks * width
    shard_rows = emb_ref.shape[0]
    tiles = rows // ROW_TILE
    groups = width // LANES
    slabs = rows // LANES
    half_rows = rows // 2
    half = slabs // 2
    total_ref = incoming

    def place(p):
        return (lax.div(p, row_n), lax.rem(p, row_n))

    barrier = pltpu.get_barrier_semaphore()

    @pl.loop(1, n)
    def _(k):
        pl.semaphore_signal(
            barrier, inc=1, device_id=place(lax.rem(me + k, n)), device_id_type=MESH
        )

    def load(piece, slot):
        @pl.loop(0, n)
        def _(p):
            start = pl.multiple_of(p * class_count + piece * narrow, LANES)
            pltpu.make_async_copy(
                weights_ref.at[:, pl.ds(start, narrow)], stage.at[slot, p], load_sem.at[slot]
            ).start()

    load(0, 0)
    emb_copy = pltpu.make_async_copy(emb_hbm, emb_ref, small_sem.at[0])
    emb_copy.start()
    labels_copy = pltpu.make_async_copy(labels_hbm, labels_ref, small_sem.at[1])
    labels_copy.start()
    load(1, 1)

    emb_copy.wait()
    emb_bf[...] = emb_ref[...].astype(jnp.bfloat16)
    mine = pl.ds(pl.multiple_of(my_row * shard_rows, shard_rows), shard_rows)
    examples[mine, :] = emb_bf[...]
    labels_copy.wait()
    pl.semaphore_wait(barrier, n - 1)

    @pl.loop(0, pieces)
    def _(c):
        slot = lax.rem(c, 2)
        pltpu.make_async_copy(stage.at[slot], stage.at[slot], load_sem.at[slot]).wait()
        spot = pl.ds(pl.multiple_of(me * features, features), features)
        chunk = lax.div(c, per)
        columns = pl.ds(pl.multiple_of(lax.rem(c, per) * narrow, narrow), narrow)

        def send(j):
            p = lax.rem(me + j + n // 2, n)
            outgoing[c, p] = stage[slot, p].astype(jnp.bfloat16)
            pltpu.make_async_remote_copy(
                src_ref=outgoing.at[c, p],
                dst_ref=incoming.at[chunk, spot, columns],
                send_sem=out_sem.at[c],
                recv_sem=in_sem.at[c],
                device_id=place(p),
                device_id_type=MESH,
            ).start()

        pl.loop(0, n // 2)(send)
        incoming[chunk, spot, columns] = stage[slot, me].astype(jnp.bfloat16)
        pl.loop(n // 2 + 1, n)(send)

        @pl.when(c == 0)
        def _():
            @pl.loop(1, row_n)
            def _(k):
                pltpu.make_async_remote_copy(
                    src_ref=emb_bf,
                    dst_ref=examples.at[mine],
                    send_sem=emb_out,
                    recv_sem=emb_in,
                    device_id=(my_cls, lax.rem(my_row + k, row_n)),
                    device_id_type=MESH,
                ).start()

        @pl.when(c + 2 < pieces)
        def _():
            load(c + 2, slot)

    for i in range(slabs):
        label_lanes[pl.ds(i * LANES, LANES), :] = (
            jnp.broadcast_to(labels_ref[i : i + 1, :], (LANES, LANES)).T - me * class_count
        )

    peers = pl.ds(0, (row_n - 1) * shard_rows)
    pltpu.make_async_copy(examples.at[peers], examples.at[peers], emb_in).wait()

    @pl.loop(0, tiles)
    def _(i):
        here = pl.ds(pl.multiple_of(i * ROW_TILE, ROW_TILE), ROW_TILE)
        product = lax.dot_general(
            examples[here, :],
            examples[...],
            (((1,), (1,)), ((), ())),
            preferred_element_type=jnp.float32,
        )
        gram[here, :] = (product * (rate * LOG2E)).astype(jnp.bfloat16)

    for i in range(tiles):
        here = pl.ds(i * ROW_TILE, ROW_TILE)
        turned = examples[here, :].astype(jnp.float32).T.astype(jnp.bfloat16)
        if i * ROW_TILE < half_rows:
            early_turned[:, here] = turned
        else:
            late_turned[:, pl.ds(i * ROW_TILE - half_rows, ROW_TILE)] = turned

    def reset():
        peak_lanes[...] = jnp.full_like(peak_lanes, -3.0e38)
        sum_lanes[...] = jnp.zeros_like(sum_lanes)
        pick_lanes[...] = jnp.zeros_like(pick_lanes)

    def hits(spot, offset, count):
        shifted = label_lanes[spot, :] - offset
        lane = lax.broadcasted_iota(jnp.int32, shifted.shape, 1)
        return [lane + q * LANES == shifted for q in range(count)]

    def collect(spot, offset, block):
        count = block.shape[1] // LANES
        parts = [block[:, q * LANES : (q + 1) * LANES] for q in range(count)]
        old = peak_lanes[spot, :]
        peak = functools.reduce(jnp.maximum, parts, old)
        total = sum_lanes[spot, :] * jnp.exp2(old - peak)
        picked = pick_lanes[spot, :]
        for part, hit in zip(parts, hits(spot, offset, count)):
            total = total + jnp.exp2(part - peak)
            picked = jnp.where(hit, part, picked)
        peak_lanes[spot, :] = peak
        sum_lanes[spot, :] = total
        pick_lanes[spot, :] = picked

    def residual(c, spot, earlier=False, to=None, to_spot=None):
        norm = norm_lanes[spot, :]
        at_label = hit_lanes[spot, :]
        for q, hit in enumerate(hits(spot, c * width, groups)):
            columns = slice(q * LANES, (q + 1) * LANES)
            part = logits[c, spot, columns]
            value = jnp.where(hit, at_label, jnp.exp2(part - norm)).astype(jnp.bfloat16)
            if earlier:
                value = value + total_ref[c, spot, columns]
            if to is None:
                total_ref[c, spot, columns] = value
            else:
                to[c, to_spot, columns] = value

    def share(src, dst, send_sem, recv_sem):
        @pl.loop(1, n)
        def _(k):
            pltpu.make_async_remote_copy(
                src_ref=src,
                dst_ref=dst.at[me],
                send_sem=send_sem,
                recv_sem=recv_sem,
                device_id=place(lax.rem(me + k, n)),
                device_id_type=MESH,
            ).start()

    def log_sums(first, count, sent):
        for i in range(count):
            part = pl.ds((first + i) * LANES, LANES)
            peaks = peak_lanes[part, :].T
            top = jnp.max(peaks, axis=0, keepdims=True)
            total = jnp.sum(sum_lanes[part, :].T * jnp.exp2(peaks - top), axis=0, keepdims=True)
            sent[i : i + 1, :] = top + jnp.log(total) * LOG2E

    def label_sums(first, count, sent, at):
        for i in range(count):
            part = pl.ds((first + i) * LANES, LANES)
            sent[at + i : at + i + 1, :] = jnp.sum(pick_lanes[part, :].T, axis=0, keepdims=True)

    others = pl.ds(0, n - 1)

    def wait(landed, sem):
        pltpu.make_async_copy(landed.at[others], landed.at[others], sem).wait()

    def agree(first, norms, picked):
        count = picked.shape[0]
        top = jnp.max(norms, axis=0)
        norm = top + jnp.log(jnp.sum(jnp.exp2(norms - top[None]), axis=0)) * LOG2E
        at_label = jnp.exp2(picked - norm) - 1.0
        for i in range(count):
            part = pl.ds((first + i) * LANES, LANES)
            norm_lanes[part, :] = jnp.broadcast_to(norm[i : i + 1, :], (LANES, LANES)).T
            hit_lanes[part, :] = jnp.broadcast_to(at_label[i : i + 1, :], (LANES, LANES)).T
        return norm

    def record(step, first, norm, picks):
        loss = (norm - jnp.sum(picks, axis=0)) * LN2
        for i in range(loss.shape[0]):
            columns = slice((first + i) * LANES, (first + i + 1) * LANES)
            losses_ref[step : step + 1, columns] = loss[i : i + 1, :]

    reset()

    @pl.loop(0, chunks)
    def _(c):
        for h in range(per):
            piece = c * per + h
            arrived = pl.ds(0, (n - 1) * features)
            columns = pl.ds(h * narrow, narrow)
            landed = incoming.at[c, arrived, columns]
            pltpu.make_async_copy(landed, landed, in_sem.at[piece]).wait()

            @pl.loop(0, tiles)
            def _(i):
                here = pl.ds(pl.multiple_of(i * ROW_TILE, ROW_TILE), ROW_TILE)
                logits[c, here, columns] = (
                    jnp.dot(
                        examples[here, :],
                        incoming[c, :, columns],
                        preferred_element_type=jnp.float32,
                    )
                    * LOG2E
                )

                @pl.loop(0, ROW_TILE // SUB, unroll=2)
                def _(u):
                    spot = pl.ds(pl.multiple_of(i * ROW_TILE + u * SUB, SUB), SUB)
                    collect(spot, piece * narrow, logits[c, spot, columns])

    log_sums(0, slabs, first_send.at[0])
    first_recv[0, me] = first_send[0]
    share(first_send.at[0], first_recv.at[0], first_out.at[0], first_in.at[0])
    label_sums(0, slabs, first_send.at[1], 0)
    first_recv[1, me] = first_send[1]
    share(first_send.at[1], first_recv.at[1], first_out.at[1], first_in.at[1])
    reset()
    wait(first_recv.at[0], first_in.at[0])
    first_norm = agree(0, first_recv[0], first_send[1])

    @pl.loop(0, rows // SUB, unroll=4)
    def _(u):
        residual(0, pl.ds(pl.multiple_of(u * SUB, SUB), SUB))

    for h in range(2):
        here = pl.ds(h * half_rows, half_rows)
        for c in range(chunks):
            change = jnp.dot(gram[here, :], total_ref[c], preferred_element_type=jnp.float32)
            if h == 0 and c + 1 < chunks:
                residual(c + 1, pl.ds(0, rows))
            block = logits[c, here, :] - change
            logits[c, here, :] = block
            collect(here, c * width, block)
        log_sums(h * half, half, later_send.at[h])
        label_sums(h * half, half, later_send.at[h], half)
        later_recv[h, me] = later_send[h]
        share(later_send.at[h], later_recv.at[h], later_out.at[h], later_in.at[h])

    wait(later_recv.at[0], later_in.at[0])
    early_norm = agree(0, later_recv[0, :, :half, :], later_send[0, half:, :])

    @pl.loop(0, half_rows // SUB, unroll=2)
    def _(u):
        spot = pl.ds(pl.multiple_of(u * SUB, SUB), SUB)
        for c in range(chunks):
            residual(c, spot, True)

    for c in range(chunks):
        for i in range(update_ref.shape[1] // ROW_TILE):
            here = pl.ds(i * ROW_TILE, ROW_TILE)
            update_ref[c, here, :] = -rate * jnp.dot(
                early_turned[here, :], total_ref[c, :half_rows, :], preferred_element_type=jnp.float32
            )

    wait(later_recv.at[1], later_in.at[1])
    late_norm = agree(half, later_recv[1, :, :half, :], later_send[1, half:, :])

    @pl.loop(0, half_rows // SUB, unroll=2)
    def _(u):
        spot = pl.ds(pl.multiple_of(half_rows + u * SUB, SUB), SUB)
        for c in range(chunks):
            residual(c, spot, True, late_ref, pl.ds(pl.multiple_of(u * SUB, SUB), SUB))

    wait(first_recv.at[1], first_in.at[1])
    record(0, 0, first_norm, first_recv[1])
    record(1, 0, early_norm, later_recv[0, :, half:, :])
    record(1, half, late_norm, later_recv[1, :, half:, :])
    for k in range(2):
        wait(first_recv.at[k], first_out.at[k])
        wait(later_recv.at[k], later_out.at[k])
    pltpu.make_async_copy(examples.at[peers], examples.at[peers], emb_out).wait()

    @pl.loop(0, pieces)
    def _(c):
        sent = pl.ds(0, n - 1)
        pltpu.make_async_copy(outgoing.at[c, sent], outgoing.at[c, sent], out_sem.at[c]).wait()


def update_kernel(
    rate, early_ref, turned_ref, total_ref, losses_in, out_ref, losses_ref, held, out_sem
):
    chunks, model_width, width = held.shape
    losses_ref[...] = losses_in[...]
    copies = []
    for c in range(chunks):
        for i in range(model_width // ROW_TILE):
            here = pl.ds(i * ROW_TILE, ROW_TILE)
            held[c, here, :] = early_ref[c, here, :] - rate * jnp.dot(
                turned_ref[here, :], total_ref[c], preferred_element_type=jnp.float32
            )
            copies.append(
                pltpu.make_async_copy(
                    held.at[c, here],
                    out_ref.at[here, pl.ds(c * width, width)],
                    out_sem.at[c, i],
                )
            )
            copies[-1].start()
    for copy in copies:
        copy.wait()


def fused(embeddings, weights, labels):
    cls_n, row_n = lax.axis_size("cls"), lax.axis_size("row")
    n = cls_n * row_n
    shard_rows, model_width = embeddings.shape
    rows = shard_rows * row_n
    features = weights.shape[0]
    class_count = weights.shape[1] // n
    width = max(w for w in (128, 256, 384, 512) if class_count % w == 0)
    narrow = 256 if width % 256 == 0 else LANES
    chunks = class_count // width
    pieces = class_count // narrow
    rate = learn_rate / rows
    slabs = rows // LANES
    half_rows = rows // 2
    vmem = pl.BlockSpec(memory_space=pltpu.VMEM)
    hbm = pl.BlockSpec(memory_space=pltpu.HBM)
    dma = pltpu.SemaphoreType.DMA
    lanes = pltpu.VMEM((rows, LANES), jnp.float32)
    operands = (embeddings, weights, labels.reshape(slabs, LANES))
    early, late, turned, losses = pl.pallas_call(
        functools.partial(exchange_kernel, cls_n, row_n, rate),
        out_shape=(
            jax.ShapeDtypeStruct((chunks, model_width, width), jnp.float32),
            jax.ShapeDtypeStruct((chunks, half_rows, width), jnp.bfloat16),
            jax.ShapeDtypeStruct((model_width, half_rows), jnp.bfloat16),
            jax.ShapeDtypeStruct((STEPS, rows), jnp.float32),
        ),
        in_specs=[hbm, hbm, hbm],
        out_specs=(vmem, vmem, vmem, vmem),
        scratch_shapes=[
            pltpu.VMEM((2, n, features, narrow), jnp.float32),
            pltpu.VMEM((pieces, n, features, narrow), jnp.bfloat16),
            pltpu.VMEM((chunks, n * features, width), jnp.bfloat16),
            pltpu.VMEM((rows, LANES), jnp.int32),
            pltpu.VMEM((chunks, rows, width), jnp.float32),
            pltpu.VMEM((rows, rows), jnp.bfloat16),
            pltpu.VMEM((rows, model_width), jnp.bfloat16),
            pltpu.VMEM((model_width, half_rows), jnp.bfloat16),
            pltpu.VMEM((shard_rows, model_width), jnp.float32),
            pltpu.VMEM((shard_rows, model_width), jnp.bfloat16),
            pltpu.VMEM((slabs, LANES), jnp.int32),
            lanes,
            lanes,
            lanes,
            lanes,
            lanes,
            pltpu.VMEM((2, slabs, LANES), jnp.float32),
            pltpu.VMEM((2, n, slabs, LANES), jnp.float32),
            pltpu.VMEM((2, slabs, LANES), jnp.float32),
            pltpu.VMEM((2, n, slabs, LANES), jnp.float32),
            dma((2,)),
            dma((2,)),
            dma((pieces,)),
            dma((pieces,)),
            dma,
            dma,
            dma((2,)),
            dma((2,)),
            dma((2,)),
            dma((2,)),
        ],
        compiler_params=pltpu.CompilerParams(
            collective_id=0, has_side_effects=True, vmem_limit_bytes=KERNEL_VMEM
        ),
    )(*(pltpu.with_memory_space_constraint(x, pltpu.HBM) for x in operands))
    update, losses = pl.pallas_call(
        functools.partial(update_kernel, rate),
        out_shape=(
            jax.ShapeDtypeStruct((model_width, class_count), jnp.float32),
            jax.ShapeDtypeStruct((STEPS, rows), jnp.float32),
        ),
        in_specs=[vmem, vmem, vmem, vmem],
        out_specs=(hbm, vmem),
        scratch_shapes=[
            pltpu.VMEM((chunks, model_width, width), jnp.float32),
            dma((chunks, model_width // ROW_TILE)),
        ],
        compiler_params=pltpu.CompilerParams(vmem_limit_bytes=UPDATE_VMEM),
    )(early, turned, late, losses)
    return update, losses


def shards(embeddings, weights, labels):
    rows = embeddings.shape[0] * lax.axis_size("row")
    square = rows == embeddings.shape[1]
    if STEPS == 2 and square and weights.shape[0] % 16 == 0:
        return fused(embeddings, weights, labels)
    peer_count = lax.axis_size(("cls", "row"))
    examples = lax.all_gather(embeddings.astype(jnp.bfloat16), "row", axis=0, tiled=True)
    row_count = examples.shape[0]
    feature_rows = weights.shape[0]
    class_count = weights.shape[1] // peer_count
    offset = lax.axis_index(("cls", "row")) * class_count
    columns = lax.broadcasted_iota(jnp.int32, (1, class_count), 1) + offset
    label_hit = columns == labels[:, None]
    pieces = weights.astype(jnp.bfloat16).reshape(feature_rows, peer_count, class_count)
    block_weights = lax.all_to_all(
        pieces.transpose(1, 0, 2), ("cls", "row"), split_axis=0, concat_axis=0, tiled=True
    )
    flat_weights = block_weights.reshape(peer_count * feature_rows, class_count)
    first_logits = jnp.dot(examples, flat_weights, preferred_element_type=jnp.float32)
    rate = learn_rate / row_count
    gram = lax.dot_general(
        examples, examples, (((1,), (1,)), ((), ())), preferred_element_type=jnp.float32
    ).astype(jnp.bfloat16)
    total = None
    loss_rows = []
    for step_index in range(STEPS):
        logits = first_logits
        if step_index > 0:
            logits = logits - rate * jnp.dot(gram, total, preferred_element_type=jnp.float32)
        local_peak = jnp.max(logits, axis=1)
        local_total = jnp.sum(jnp.exp(logits - local_peak[:, None]), axis=1)
        local_picked = jnp.sum(jnp.where(label_hit, logits, 0.0), axis=1)
        stats = lax.all_gather(
            jnp.stack([local_peak, local_total, local_picked]), ("cls", "row"), axis=0
        )
        row_peak = jnp.max(stats[:, 0], axis=0)
        row_total = jnp.sum(stats[:, 1] * jnp.exp(stats[:, 0] - row_peak[None, :]), axis=0)
        picked = jnp.sum(stats[:, 2], axis=0)
        log_norm = row_peak + jnp.log(row_total)
        loss_rows.append(log_norm - picked)
        onehot = jnp.where(label_hit, 1.0, 0.0)
        residual = jnp.exp(logits - log_norm[:, None]) - onehot
        if total is not None:
            residual = residual + total.astype(jnp.float32)
        total = residual.astype(jnp.bfloat16)
    update = lax.dot_general(
        examples, total, (((0,), (0,)), ((), ())), preferred_element_type=jnp.float32
    )
    return (-rate * update, jnp.stack(loss_rows))


def solution(mesh):
    placed = (P("row", None), P(("cls", "row"), None), P())
    return jax.shard_map(
        shards,
        mesh=mesh,
        in_specs=placed,
        out_specs=(P(None, ("cls", "row")), P()),
        check_vma=False,
    )
```

```python
import functools

import jax
import jax.numpy as jnp
from jax import lax
from jax.experimental import pallas as pl
from jax.experimental.pallas import tpu as pltpu
from jax.sharding import PartitionSpec as P

STEPS = 2


learn_rate = 2.0

MESH = pl.DeviceIdType.MESH
LANES = 128
ROW_TILE = 256
SUB = 32
LOG2E = 1.4426950408889634
LN2 = 0.6931471805599453
KERNEL_VMEM = 40 * 1024 * 1024
UPDATE_VMEM = 24 * 1024 * 1024


def exchange_kernel(
    cls_n,
    row_n,
    rate,
    emb_hbm,
    weights_ref,
    labels_hbm,
    update_ref,
    late_ref,
    late_turned,
    losses_ref,
    stage,
    outgoing,
    incoming,
    label_lanes,
    logits,
    gram,
    examples,
    early_turned,
    emb_ref,
    emb_bf,
    labels_ref,
    peak_lanes,
    sum_lanes,
    pick_lanes,
    norm_lanes,
    hit_lanes,
    first_send,
    first_recv,
    later_send,
    later_recv,
    load_sem,
    small_sem,
    out_sem,
    in_sem,
    emb_out,
    emb_in,
    first_out,
    first_in,
    later_out,
    later_in,
):
    n = cls_n * row_n
    my_cls, my_row = lax.axis_index("cls"), lax.axis_index("row")
    me = my_cls * row_n + my_row
    chunks, rows, width = logits.shape
    pieces, _, features, narrow = outgoing.shape
    per = width // narrow
    class_count = chunks * width
    shard_rows = emb_ref.shape[0]
    tiles = rows // ROW_TILE
    groups = width // LANES
    slabs = rows // LANES
    half_rows = rows // 2
    half = slabs // 2
    total_ref = incoming

    def place(p):
        return (lax.div(p, row_n), lax.rem(p, row_n))

    barrier = pltpu.get_barrier_semaphore()

    @pl.loop(1, n)
    def _(k):
        pl.semaphore_signal(
            barrier, inc=1, device_id=place(lax.rem(me + k, n)), device_id_type=MESH
        )

    def load(piece, slot):
        @pl.loop(0, n)
        def _(p):
            start = pl.multiple_of(p * class_count + piece * narrow, LANES)
            pltpu.make_async_copy(
                weights_ref.at[:, pl.ds(start, narrow)], stage.at[slot, p], load_sem.at[slot]
            ).start()

    load(0, 0)
    emb_copy = pltpu.make_async_copy(emb_hbm, emb_ref, small_sem.at[0])
    emb_copy.start()
    labels_copy = pltpu.make_async_copy(labels_hbm, labels_ref, small_sem.at[1])
    labels_copy.start()
    load(1, 1)

    emb_copy.wait()
    emb_bf[...] = emb_ref[...].astype(jnp.bfloat16)
    mine = pl.ds(pl.multiple_of(my_row * shard_rows, shard_rows), shard_rows)
    examples[mine, :] = emb_bf[...]
    labels_copy.wait()
    pl.semaphore_wait(barrier, n - 1)

    @pl.loop(0, pieces)
    def _(c):
        slot = lax.rem(c, 2)
        pltpu.make_async_copy(stage.at[slot], stage.at[slot], load_sem.at[slot]).wait()
        spot = pl.ds(pl.multiple_of(me * features, features), features)
        chunk = lax.div(c, per)
        columns = pl.ds(pl.multiple_of(lax.rem(c, per) * narrow, narrow), narrow)

        def send(j):
            p = lax.rem(me + j + n // 2, n)
            outgoing[c, p] = stage[slot, p].astype(jnp.bfloat16)
            pltpu.make_async_remote_copy(
                src_ref=outgoing.at[c, p],
                dst_ref=incoming.at[chunk, spot, columns],
                send_sem=out_sem.at[c],
                recv_sem=in_sem.at[c],
                device_id=place(p),
                device_id_type=MESH,
            ).start()

        pl.loop(0, n // 2)(send)
        incoming[chunk, spot, columns] = stage[slot, me].astype(jnp.bfloat16)
        pl.loop(n // 2 + 1, n)(send)

        @pl.when(c == 0)
        def _():
            @pl.loop(1, row_n)
            def _(k):
                pltpu.make_async_remote_copy(
                    src_ref=emb_bf,
                    dst_ref=examples.at[mine],
                    send_sem=emb_out,
                    recv_sem=emb_in,
                    device_id=(my_cls, lax.rem(my_row + k, row_n)),
                    device_id_type=MESH,
                ).start()

        @pl.when(c + 2 < pieces)
        def _():
            load(c + 2, slot)

    for i in range(slabs):
        label_lanes[pl.ds(i * LANES, LANES), :] = (
            jnp.broadcast_to(labels_ref[i : i + 1, :], (LANES, LANES)).T - me * class_count
        )

    peers = pl.ds(0, (row_n - 1) * shard_rows)
    pltpu.make_async_copy(examples.at[peers], examples.at[peers], emb_in).wait()

    @pl.loop(0, tiles)
    def _(i):
        here = pl.ds(pl.multiple_of(i * ROW_TILE, ROW_TILE), ROW_TILE)
        product = lax.dot_general(
            examples[here, :],
            examples[...],
            (((1,), (1,)), ((), ())),
            preferred_element_type=jnp.float32,
        )
        gram[here, :] = (product * (rate * LOG2E)).astype(jnp.bfloat16)

    for i in range(tiles):
        here = pl.ds(i * ROW_TILE, ROW_TILE)
        turned = examples[here, :].astype(jnp.float32).T.astype(jnp.bfloat16)
        if i * ROW_TILE < half_rows:
            early_turned[:, here] = turned
        else:
            late_turned[:, pl.ds(i * ROW_TILE - half_rows, ROW_TILE)] = turned

    def reset():
        peak_lanes[...] = jnp.full_like(peak_lanes, -3.0e38)
        sum_lanes[...] = jnp.zeros_like(sum_lanes)
        pick_lanes[...] = jnp.zeros_like(pick_lanes)

    def hits(spot, offset, count):
        shifted = label_lanes[spot, :] - offset
        lane = lax.broadcasted_iota(jnp.int32, shifted.shape, 1)
        return [lane + q * LANES == shifted for q in range(count)]

    def collect(spot, offset, block):
        count = block.shape[1] // LANES
        parts = [block[:, q * LANES : (q + 1) * LANES] for q in range(count)]
        old = peak_lanes[spot, :]
        peak = functools.reduce(jnp.maximum, parts, old)
        total = sum_lanes[spot, :] * jnp.exp2(old - peak)
        picked = pick_lanes[spot, :]
        for part, hit in zip(parts, hits(spot, offset, count)):
            total = total + jnp.exp2(part - peak)
            picked = jnp.where(hit, part, picked)
        peak_lanes[spot, :] = peak
        sum_lanes[spot, :] = total
        pick_lanes[spot, :] = picked

    def residual(c, spot, to, to_spot):
        norm = norm_lanes[spot, :]
        at_label = hit_lanes[spot, :]
        for q, hit in enumerate(hits(spot, c * width, groups)):
            columns = slice(q * LANES, (q + 1) * LANES)
            part = logits[c, spot, columns]
            value = jnp.where(hit, at_label, jnp.exp2(part - norm)).astype(jnp.bfloat16)
            to[c, to_spot, columns] = value + total_ref[c, spot, columns]

    def share(src, dst, send_sem, recv_sem):
        for k in range(1, n):
            pltpu.make_async_remote_copy(
                src_ref=src,
                dst_ref=dst.at[me],
                send_sem=send_sem,
                recv_sem=recv_sem,
                device_id=place(lax.rem(me + k, n)),
                device_id_type=MESH,
            ).start()

    def log_sums(first, count, sent):
        for i in range(count):
            part = pl.ds((first + i) * LANES, LANES)
            peaks = peak_lanes[part, :].T
            top = jnp.max(peaks, axis=0, keepdims=True)
            total = jnp.sum(sum_lanes[part, :].T * jnp.exp2(peaks - top), axis=0, keepdims=True)
            sent[i : i + 1, :] = top + jnp.log(total) * LOG2E

    def label_sums(first, count, sent, at):
        for i in range(count):
            part = pl.ds((first + i) * LANES, LANES)
            sent[at + i : at + i + 1, :] = jnp.sum(pick_lanes[part, :].T, axis=0, keepdims=True)

    others = pl.ds(0, n - 1)

    def wait(landed, sem):
        pltpu.make_async_copy(landed.at[others], landed.at[others], sem).wait()

    def agree(first, norms, picked, local=None):
        count = picked.shape[0]
        top = jnp.max(norms, axis=0)
        norm = top + jnp.log(jnp.sum(jnp.exp2(norms - top[None]), axis=0)) * LOG2E
        at_label = jnp.exp2(picked - norm) - 1.0
        factor = norm if local is None else jnp.exp2(local - norm)
        for i in range(count):
            part = pl.ds((first + i) * LANES, LANES)
            norm_lanes[part, :] = jnp.broadcast_to(factor[i : i + 1, :], (LANES, LANES)).T
            hit_lanes[part, :] = jnp.broadcast_to(at_label[i : i + 1, :], (LANES, LANES)).T
        return norm

    def relative(c, spot):
        local = norm_lanes[spot, :]
        for q, hit in enumerate(hits(spot, c * width, groups)):
            columns = slice(q * LANES, (q + 1) * LANES)
            value = jnp.exp2(logits[c, spot, columns] - local)
            total_ref[c, spot, columns] = jnp.where(hit, -1.0, value).astype(jnp.bfloat16)

    def rescale(c, spot):
        factor = norm_lanes[spot, :].astype(jnp.bfloat16)
        at_label = hit_lanes[spot, :].astype(jnp.bfloat16)
        for q in range(groups):
            columns = slice(q * LANES, (q + 1) * LANES)
            value = total_ref[c, spot, columns]
            total_ref[c, spot, columns] = jnp.where(value < 0, at_label, value * factor)

    def record(step, first, norm, picks):
        loss = (norm - jnp.sum(picks, axis=0)) * LN2
        for i in range(loss.shape[0]):
            columns = slice((first + i) * LANES, (first + i + 1) * LANES)
            losses_ref[step : step + 1, columns] = loss[i : i + 1, :]

    reset()

    @pl.loop(0, chunks)
    def _(c):
        for h in range(per):
            piece = c * per + h
            arrived = pl.ds(0, (n - 1) * features)
            columns = pl.ds(h * narrow, narrow)
            landed = incoming.at[c, arrived, columns]
            pltpu.make_async_copy(landed, landed, in_sem.at[piece]).wait()

            @pl.loop(0, tiles)
            def _(i):
                here = pl.ds(pl.multiple_of(i * ROW_TILE, ROW_TILE), ROW_TILE)
                logits[c, here, columns] = (
                    jnp.dot(
                        examples[here, :],
                        incoming[c, :, columns],
                        preferred_element_type=jnp.float32,
                    )
                    * LOG2E
                )

                @pl.loop(0, ROW_TILE // SUB, unroll=2)
                def _(u):
                    spot = pl.ds(pl.multiple_of(i * ROW_TILE + u * SUB, SUB), SUB)
                    collect(spot, piece * narrow, logits[c, spot, columns])

    log_sums(0, slabs, first_send.at[0])
    first_recv[0, me] = first_send[0]
    share(first_send.at[0], first_recv.at[0], first_out.at[0], first_in.at[0])
    label_sums(0, slabs, first_send.at[1], 0)
    first_recv[1, me] = first_send[1]
    share(first_send.at[1], first_recv.at[1], first_out.at[1], first_in.at[1])
    reset()
    for i in range(slabs):
        local = jnp.broadcast_to(first_send[0, i : i + 1, :], (LANES, LANES))
        norm_lanes[pl.ds(i * LANES, LANES), :] = local.T

    @pl.loop(0, rows // SUB, unroll=2)
    def _(u):
        for c in range(chunks):
            relative(c, pl.ds(pl.multiple_of(u * SUB, SUB), SUB))

    wait(first_recv.at[0], first_in.at[0])
    first_norm = agree(0, first_recv[0], first_send[1], first_send[0])
    rescale(0, pl.ds(0, rows))

    for h in range(2):
        here = pl.ds(h * half_rows, half_rows)
        for c in range(chunks):
            change = jnp.dot(gram[here, :], total_ref[c], preferred_element_type=jnp.float32)
            if h == 0 and c + 1 < chunks:
                rescale(c + 1, pl.ds(0, rows))
            block = logits[c, here, :] - change
            logits[c, here, :] = block
            collect(here, c * width, block)
        log_sums(h * half, half, later_send.at[h])
        label_sums(h * half, half, later_send.at[h], half)
        later_recv[h, me] = later_send[h]
        share(later_send.at[h], later_recv.at[h], later_out.at[h], later_in.at[h])

    wait(later_recv.at[0], later_in.at[0])
    early_norm = agree(0, later_recv[0, :, :half, :], later_send[0, half:, :])

    @pl.loop(0, half_rows // SUB, unroll=2)
    def _(u):
        spot = pl.ds(pl.multiple_of(u * SUB, SUB), SUB)
        for c in range(chunks):
            residual(c, spot, total_ref, spot)

    for c in range(chunks):
        for i in range(update_ref.shape[1] // ROW_TILE):
            here = pl.ds(i * ROW_TILE, ROW_TILE)
            update_ref[c, here, :] = -rate * jnp.dot(
                early_turned[here, :], total_ref[c, :half_rows, :], preferred_element_type=jnp.float32
            )

    wait(later_recv.at[1], later_in.at[1])
    late_norm = agree(half, later_recv[1, :, :half, :], later_send[1, half:, :])

    @pl.loop(0, half_rows // SUB, unroll=2)
    def _(u):
        spot = pl.ds(pl.multiple_of(half_rows + u * SUB, SUB), SUB)
        for c in range(chunks):
            residual(c, spot, late_ref, pl.ds(pl.multiple_of(u * SUB, SUB), SUB))

    wait(first_recv.at[1], first_in.at[1])
    record(0, 0, first_norm, first_recv[1])
    record(1, 0, early_norm, later_recv[0, :, half:, :])
    record(1, half, late_norm, later_recv[1, :, half:, :])
    for k in range(2):
        wait(first_recv.at[k], first_out.at[k])
        wait(later_recv.at[k], later_out.at[k])
    pltpu.make_async_copy(examples.at[peers], examples.at[peers], emb_out).wait()

    @pl.loop(0, pieces)
    def _(c):
        sent = pl.ds(0, n - 1)
        pltpu.make_async_copy(outgoing.at[c, sent], outgoing.at[c, sent], out_sem.at[c]).wait()


def update_kernel(
    rate, early_ref, turned_ref, total_ref, losses_in, out_ref, losses_ref, held, out_sem
):
    chunks, model_width, width = held.shape
    losses_ref[...] = losses_in[...]
    copies = []
    for c in range(chunks):
        for i in range(model_width // ROW_TILE):
            here = pl.ds(i * ROW_TILE, ROW_TILE)
            held[c, here, :] = early_ref[c, here, :] - rate * jnp.dot(
                turned_ref[here, :], total_ref[c], preferred_element_type=jnp.float32
            )
            copies.append(
                pltpu.make_async_copy(
                    held.at[c, here],
                    out_ref.at[here, pl.ds(c * width, width)],
                    out_sem.at[c, i],
                )
            )
            copies[-1].start()
    for copy in copies:
        copy.wait()


def fused(embeddings, weights, labels):
    cls_n, row_n = lax.axis_size("cls"), lax.axis_size("row")
    n = cls_n * row_n
    shard_rows, model_width = embeddings.shape
    rows = shard_rows * row_n
    features = weights.shape[0]
    class_count = weights.shape[1] // n
    width = max(w for w in (128, 256, 384, 512) if class_count % w == 0)
    narrow = 256 if width % 256 == 0 else LANES
    chunks = class_count // width
    pieces = class_count // narrow
    rate = learn_rate / rows
    slabs = rows // LANES
    half_rows = rows // 2
    vmem = pl.BlockSpec(memory_space=pltpu.VMEM)
    hbm = pl.BlockSpec(memory_space=pltpu.HBM)
    dma = pltpu.SemaphoreType.DMA
    lanes = pltpu.VMEM((rows, LANES), jnp.float32)
    operands = (embeddings, weights, labels.reshape(slabs, LANES))
    early, late, turned, losses = pl.pallas_call(
        functools.partial(exchange_kernel, cls_n, row_n, rate),
        out_shape=(
            jax.ShapeDtypeStruct((chunks, model_width, width), jnp.float32),
            jax.ShapeDtypeStruct((chunks, half_rows, width), jnp.bfloat16),
            jax.ShapeDtypeStruct((model_width, half_rows), jnp.bfloat16),
            jax.ShapeDtypeStruct((STEPS, rows), jnp.float32),
        ),
        in_specs=[hbm, hbm, hbm],
        out_specs=(vmem, vmem, vmem, vmem),
        scratch_shapes=[
            pltpu.VMEM((2, n, features, narrow), jnp.float32),
            pltpu.VMEM((pieces, n, features, narrow), jnp.bfloat16),
            pltpu.VMEM((chunks, n * features, width), jnp.bfloat16),
            pltpu.VMEM((rows, LANES), jnp.int32),
            pltpu.VMEM((chunks, rows, width), jnp.float32),
            pltpu.VMEM((rows, rows), jnp.bfloat16),
            pltpu.VMEM((rows, model_width), jnp.bfloat16),
            pltpu.VMEM((model_width, half_rows), jnp.bfloat16),
            pltpu.VMEM((shard_rows, model_width), jnp.float32),
            pltpu.VMEM((shard_rows, model_width), jnp.bfloat16),
            pltpu.VMEM((slabs, LANES), jnp.int32),
            lanes,
            lanes,
            lanes,
            lanes,
            lanes,
            pltpu.VMEM((2, slabs, LANES), jnp.float32),
            pltpu.VMEM((2, n, slabs, LANES), jnp.float32),
            pltpu.VMEM((2, slabs, LANES), jnp.float32),
            pltpu.VMEM((2, n, slabs, LANES), jnp.float32),
            dma((2,)),
            dma((2,)),
            dma((pieces,)),
            dma((pieces,)),
            dma,
            dma,
            dma((2,)),
            dma((2,)),
            dma((2,)),
            dma((2,)),
        ],
        compiler_params=pltpu.CompilerParams(
            collective_id=0, has_side_effects=True, vmem_limit_bytes=KERNEL_VMEM
        ),
    )(*(pltpu.with_memory_space_constraint(x, pltpu.HBM) for x in operands))
    update, losses = pl.pallas_call(
        functools.partial(update_kernel, rate),
        out_shape=(
            jax.ShapeDtypeStruct((model_width, class_count), jnp.float32),
            jax.ShapeDtypeStruct((STEPS, rows), jnp.float32),
        ),
        in_specs=[vmem, vmem, vmem, vmem],
        out_specs=(hbm, vmem),
        scratch_shapes=[
            pltpu.VMEM((chunks, model_width, width), jnp.float32),
            dma((chunks, model_width // ROW_TILE)),
        ],
        compiler_params=pltpu.CompilerParams(vmem_limit_bytes=UPDATE_VMEM),
    )(early, turned, late, losses)
    return update, losses


def shards(embeddings, weights, labels):
    rows = embeddings.shape[0] * lax.axis_size("row")
    square = rows == embeddings.shape[1]
    if STEPS == 2 and square and weights.shape[0] % 16 == 0:
        return fused(embeddings, weights, labels)
    peer_count = lax.axis_size(("cls", "row"))
    examples = lax.all_gather(embeddings.astype(jnp.bfloat16), "row", axis=0, tiled=True)
    row_count = examples.shape[0]
    feature_rows = weights.shape[0]
    class_count = weights.shape[1] // peer_count
    offset = lax.axis_index(("cls", "row")) * class_count
    columns = lax.broadcasted_iota(jnp.int32, (1, class_count), 1) + offset
    label_hit = columns == labels[:, None]
    pieces = weights.astype(jnp.bfloat16).reshape(feature_rows, peer_count, class_count)
    block_weights = lax.all_to_all(
        pieces.transpose(1, 0, 2), ("cls", "row"), split_axis=0, concat_axis=0, tiled=True
    )
    flat_weights = block_weights.reshape(peer_count * feature_rows, class_count)
    first_logits = jnp.dot(examples, flat_weights, preferred_element_type=jnp.float32)
    rate = learn_rate / row_count
    gram = lax.dot_general(
        examples, examples, (((1,), (1,)), ((), ())), preferred_element_type=jnp.float32
    ).astype(jnp.bfloat16)
    total = None
    loss_rows = []
    for step_index in range(STEPS):
        logits = first_logits
        if step_index > 0:
            logits = logits - rate * jnp.dot(gram, total, preferred_element_type=jnp.float32)
        local_peak = jnp.max(logits, axis=1)
        local_total = jnp.sum(jnp.exp(logits - local_peak[:, None]), axis=1)
        local_picked = jnp.sum(jnp.where(label_hit, logits, 0.0), axis=1)
        stats = lax.all_gather(
            jnp.stack([local_peak, local_total, local_picked]), ("cls", "row"), axis=0
        )
        row_peak = jnp.max(stats[:, 0], axis=0)
        row_total = jnp.sum(stats[:, 1] * jnp.exp(stats[:, 0] - row_peak[None, :]), axis=0)
        picked = jnp.sum(stats[:, 2], axis=0)
        log_norm = row_peak + jnp.log(row_total)
        loss_rows.append(log_norm - picked)
        onehot = jnp.where(label_hit, 1.0, 0.0)
        residual = jnp.exp(logits - log_norm[:, None]) - onehot
        if total is not None:
            residual = residual + total.astype(jnp.float32)
        total = residual.astype(jnp.bfloat16)
    update = lax.dot_general(
        examples, total, (((0,), (0,)), ((), ())), preferred_element_type=jnp.float32
    )
    return (-rate * update, jnp.stack(loss_rows))


def solution(mesh):
    placed = (P("row", None), P(("cls", "row"), None), P())
    return jax.shard_map(
        shards,
        mesh=mesh,
        in_specs=placed,
        out_specs=(P(None, ("cls", "row")), P()),
        check_vma=False,
    )
```

```python
import functools

import jax
import jax.numpy as jnp
from jax import lax
from jax.experimental import pallas as pl
from jax.experimental.pallas import tpu as pltpu
from jax.sharding import PartitionSpec as P

STEPS = 2


learn_rate = 2.0

MESH = pl.DeviceIdType.MESH
LANES = 128
ROW_TILE = 256
SUB = 32
LOG2E = 1.4426950408889634
LN2 = 0.6931471805599453
KERNEL_VMEM = 40 * 1024 * 1024
UPDATE_VMEM = 24 * 1024 * 1024


def exchange_kernel(
    cls_n,
    row_n,
    rate,
    emb_hbm,
    weights_ref,
    labels_hbm,
    update_ref,
    late_ref,
    late_turned,
    losses_ref,
    stage,
    outgoing,
    incoming,
    label_lanes,
    logits,
    gram,
    examples,
    early_turned,
    emb_ref,
    emb_bf,
    labels_ref,
    peak_lanes,
    sum_lanes,
    pick_lanes,
    norm_lanes,
    hit_lanes,
    first_send,
    first_recv,
    later_send,
    later_recv,
    load_sem,
    small_sem,
    out_sem,
    in_sem,
    emb_out,
    emb_in,
    first_out,
    first_in,
    later_out,
    later_in,
):
    n = cls_n * row_n
    my_cls, my_row = lax.axis_index("cls"), lax.axis_index("row")
    me = my_cls * row_n + my_row
    chunks, rows, width = logits.shape
    pieces, _, features, narrow = outgoing.shape
    per = width // narrow
    class_count = chunks * width
    shard_rows = emb_ref.shape[0]
    tiles = rows // ROW_TILE
    groups = width // LANES
    slabs = rows // LANES
    half_rows = rows // 2
    half = slabs // 2
    total_ref = incoming

    def place(p):
        return (lax.div(p, row_n), lax.rem(p, row_n))

    barrier = pltpu.get_barrier_semaphore()

    @pl.loop(1, n)
    def _(k):
        pl.semaphore_signal(
            barrier, inc=1, device_id=place(lax.rem(me + k, n)), device_id_type=MESH
        )

    def load(piece, slot):
        @pl.loop(0, n)
        def _(p):
            start = pl.multiple_of(p * class_count + piece * narrow, LANES)
            pltpu.make_async_copy(
                weights_ref.at[:, pl.ds(start, narrow)], stage.at[slot, p], load_sem.at[slot]
            ).start()

    load(0, 0)
    emb_copy = pltpu.make_async_copy(emb_hbm, emb_ref, small_sem.at[0])
    emb_copy.start()
    labels_copy = pltpu.make_async_copy(labels_hbm, labels_ref, small_sem.at[1])
    labels_copy.start()
    load(1, 1)

    emb_copy.wait()
    emb_bf[...] = emb_ref[...].astype(jnp.bfloat16)
    mine = pl.ds(pl.multiple_of(my_row * shard_rows, shard_rows), shard_rows)
    examples[mine, :] = emb_bf[...]
    labels_copy.wait()
    pl.semaphore_wait(barrier, n - 1)

    @pl.loop(0, pieces)
    def _(c):
        slot = lax.rem(c, 2)
        pltpu.make_async_copy(stage.at[slot], stage.at[slot], load_sem.at[slot]).wait()
        spot = pl.ds(pl.multiple_of(me * features, features), features)
        chunk = lax.div(c, per)
        columns = pl.ds(pl.multiple_of(lax.rem(c, per) * narrow, narrow), narrow)

        def send(j):
            p = lax.rem(me + j + n // 2, n)
            outgoing[c, p] = stage[slot, p].astype(jnp.bfloat16)
            pltpu.make_async_remote_copy(
                src_ref=outgoing.at[c, p],
                dst_ref=incoming.at[chunk, spot, columns],
                send_sem=out_sem.at[c],
                recv_sem=in_sem.at[c],
                device_id=place(p),
                device_id_type=MESH,
            ).start()

        pl.loop(0, n // 2)(send)
        incoming[chunk, spot, columns] = stage[slot, me].astype(jnp.bfloat16)
        pl.loop(n // 2 + 1, n)(send)

        @pl.when(c == 0)
        def _():
            @pl.loop(1, row_n)
            def _(k):
                pltpu.make_async_remote_copy(
                    src_ref=emb_bf,
                    dst_ref=examples.at[mine],
                    send_sem=emb_out,
                    recv_sem=emb_in,
                    device_id=(my_cls, lax.rem(my_row + k, row_n)),
                    device_id_type=MESH,
                ).start()

        @pl.when(c + 2 < pieces)
        def _():
            load(c + 2, slot)

    for i in range(slabs):
        label_lanes[pl.ds(i * LANES, LANES), :] = (
            jnp.broadcast_to(labels_ref[i : i + 1, :], (LANES, LANES)).T - me * class_count
        )

    peers = pl.ds(0, (row_n - 1) * shard_rows)
    pltpu.make_async_copy(examples.at[peers], examples.at[peers], emb_in).wait()

    @pl.loop(0, tiles)
    def _(i):
        here = pl.ds(pl.multiple_of(i * ROW_TILE, ROW_TILE), ROW_TILE)
        product = lax.dot_general(
            examples[here, :],
            examples[...],
            (((1,), (1,)), ((), ())),
            preferred_element_type=jnp.float32,
        )
        gram[here, :] = (product * (rate * LOG2E)).astype(jnp.bfloat16)

    for i in range(tiles):
        here = pl.ds(i * ROW_TILE, ROW_TILE)
        turned = examples[here, :].astype(jnp.float32).T.astype(jnp.bfloat16)
        if i * ROW_TILE < half_rows:
            early_turned[:, here] = turned
        else:
            late_turned[:, pl.ds(i * ROW_TILE - half_rows, ROW_TILE)] = turned

    def reset():
        peak_lanes[...] = jnp.full_like(peak_lanes, -3.0e38)
        sum_lanes[...] = jnp.zeros_like(sum_lanes)
        pick_lanes[...] = jnp.zeros_like(pick_lanes)

    def hits(spot, offset, count):
        shifted = label_lanes[spot, :] - offset
        lane = lax.broadcasted_iota(jnp.int32, shifted.shape, 1)
        return [lane + q * LANES == shifted for q in range(count)]

    def collect(spot, offset, block):
        count = block.shape[1] // LANES
        parts = [block[:, q * LANES : (q + 1) * LANES] for q in range(count)]
        old = peak_lanes[spot, :]
        peak = functools.reduce(jnp.maximum, parts, old)
        total = sum_lanes[spot, :] * jnp.exp2(old - peak)
        picked = pick_lanes[spot, :]
        for part, hit in zip(parts, hits(spot, offset, count)):
            total = total + jnp.exp2(part - peak)
            picked = jnp.where(hit, part, picked)
        peak_lanes[spot, :] = peak
        sum_lanes[spot, :] = total
        pick_lanes[spot, :] = picked

    def residual(c, spot, to, to_spot):
        norm = norm_lanes[spot, :]
        at_label = hit_lanes[spot, :]
        for q, hit in enumerate(hits(spot, c * width, groups)):
            columns = slice(q * LANES, (q + 1) * LANES)
            part = logits[c, spot, columns]
            value = jnp.where(hit, at_label, jnp.exp2(part - norm)).astype(jnp.bfloat16)
            to[c, to_spot, columns] = value + total_ref[c, spot, columns]

    def share(src, dst, send_sem, recv_sem):
        @pl.loop(1, n)
        def _(k):
            pltpu.make_async_remote_copy(
                src_ref=src,
                dst_ref=dst.at[me],
                send_sem=send_sem,
                recv_sem=recv_sem,
                device_id=place(lax.rem(me + k, n)),
                device_id_type=MESH,
            ).start()

    def log_sums(first, count, sent):
        for i in range(count):
            part = pl.ds((first + i) * LANES, LANES)
            peaks = peak_lanes[part, :].T
            top = jnp.max(peaks, axis=0, keepdims=True)
            total = jnp.sum(sum_lanes[part, :].T * jnp.exp2(peaks - top), axis=0, keepdims=True)
            sent[i : i + 1, :] = top + jnp.log(total) * LOG2E

    def label_sums(first, count, sent, at):
        for i in range(count):
            part = pl.ds((first + i) * LANES, LANES)
            sent[at + i : at + i + 1, :] = jnp.sum(pick_lanes[part, :].T, axis=0, keepdims=True)

    others = pl.ds(0, n - 1)

    def wait(landed, sem):
        pltpu.make_async_copy(landed.at[others], landed.at[others], sem).wait()

    def agree(first, norms, picked, local=None):
        count = picked.shape[0]
        top = jnp.max(norms, axis=0)
        norm = top + jnp.log(jnp.sum(jnp.exp2(norms - top[None]), axis=0)) * LOG2E
        at_label = jnp.exp2(picked - norm) - 1.0
        factor = norm if local is None else jnp.exp2(local - norm)
        for i in range(count):
            part = pl.ds((first + i) * LANES, LANES)
            norm_lanes[part, :] = jnp.broadcast_to(factor[i : i + 1, :], (LANES, LANES)).T
            hit_lanes[part, :] = jnp.broadcast_to(at_label[i : i + 1, :], (LANES, LANES)).T
        return norm

    def relative(c, spot):
        local = norm_lanes[spot, :]
        for q, hit in enumerate(hits(spot, c * width, groups)):
            columns = slice(q * LANES, (q + 1) * LANES)
            value = jnp.exp2(logits[c, spot, columns] - local)
            total_ref[c, spot, columns] = jnp.where(hit, -1.0, value).astype(jnp.bfloat16)

    def rescale(c, spot):
        factor = norm_lanes[spot, :].astype(jnp.bfloat16)
        at_label = hit_lanes[spot, :].astype(jnp.bfloat16)
        for q in range(groups):
            columns = slice(q * LANES, (q + 1) * LANES)
            value = total_ref[c, spot, columns]
            total_ref[c, spot, columns] = jnp.where(value < 0, at_label, value * factor)

    def record(step, first, norm, picks):
        loss = (norm - jnp.sum(picks, axis=0)) * LN2
        for i in range(loss.shape[0]):
            columns = slice((first + i) * LANES, (first + i + 1) * LANES)
            losses_ref[step : step + 1, columns] = loss[i : i + 1, :]

    reset()

    @pl.loop(0, chunks)
    def _(c):
        for h in range(per):
            piece = c * per + h
            arrived = pl.ds(0, (n - 1) * features)
            columns = pl.ds(h * narrow, narrow)
            landed = incoming.at[c, arrived, columns]
            pltpu.make_async_copy(landed, landed, in_sem.at[piece]).wait()

            @pl.loop(0, tiles)
            def _(i):
                here = pl.ds(pl.multiple_of(i * ROW_TILE, ROW_TILE), ROW_TILE)
                logits[c, here, columns] = (
                    jnp.dot(
                        examples[here, :],
                        incoming[c, :, columns],
                        preferred_element_type=jnp.float32,
                    )
                    * LOG2E
                )

                @pl.loop(0, ROW_TILE // SUB, unroll=2)
                def _(u):
                    spot = pl.ds(pl.multiple_of(i * ROW_TILE + u * SUB, SUB), SUB)
                    collect(spot, piece * narrow, logits[c, spot, columns])

    log_sums(0, slabs, first_send.at[0])
    first_recv[0, me] = first_send[0]
    share(first_send.at[0], first_recv.at[0], first_out.at[0], first_in.at[0])
    label_sums(0, slabs, first_send.at[1], 0)
    first_recv[1, me] = first_send[1]
    share(first_send.at[1], first_recv.at[1], first_out.at[1], first_in.at[1])
    reset()
    for i in range(slabs):
        local = jnp.broadcast_to(first_send[0, i : i + 1, :], (LANES, LANES))
        norm_lanes[pl.ds(i * LANES, LANES), :] = local.T

    @pl.loop(0, rows // SUB, unroll=2)
    def _(u):
        for c in range(chunks):
            relative(c, pl.ds(pl.multiple_of(u * SUB, SUB), SUB))

    wait(first_recv.at[0], first_in.at[0])
    first_norm = agree(0, first_recv[0], first_send[1], first_send[0])
    rescale(0, pl.ds(0, rows))

    for h in range(2):
        here = pl.ds(h * half_rows, half_rows)
        for c in range(chunks):
            change = jnp.dot(gram[here, :], total_ref[c], preferred_element_type=jnp.float32)
            if h == 0 and c + 1 < chunks:
                rescale(c + 1, pl.ds(0, rows))
            block = logits[c, here, :] - change
            logits[c, here, :] = block
            collect(here, c * width, block)
        log_sums(h * half, half, later_send.at[h])
        label_sums(h * half, half, later_send.at[h], half)
        later_recv[h, me] = later_send[h]
        share(later_send.at[h], later_recv.at[h], later_out.at[h], later_in.at[h])

    wait(later_recv.at[0], later_in.at[0])
    early_norm = agree(0, later_recv[0, :, :half, :], later_send[0, half:, :])

    @pl.loop(0, half_rows // SUB, unroll=2)
    def _(u):
        spot = pl.ds(pl.multiple_of(u * SUB, SUB), SUB)
        for c in range(chunks):
            residual(c, spot, total_ref, spot)

    for c in range(chunks):
        for i in range(update_ref.shape[1] // ROW_TILE):
            here = pl.ds(i * ROW_TILE, ROW_TILE)
            update_ref[c, here, :] = -rate * jnp.dot(
                early_turned[here, :], total_ref[c, :half_rows, :], preferred_element_type=jnp.float32
            )

    wait(later_recv.at[1], later_in.at[1])
    late_norm = agree(half, later_recv[1, :, :half, :], later_send[1, half:, :])

    @pl.loop(0, half_rows // SUB, unroll=2)
    def _(u):
        spot = pl.ds(pl.multiple_of(half_rows + u * SUB, SUB), SUB)
        for c in range(chunks):
            residual(c, spot, late_ref, pl.ds(pl.multiple_of(u * SUB, SUB), SUB))

    wait(first_recv.at[1], first_in.at[1])
    record(0, 0, first_norm, first_recv[1])
    record(1, 0, early_norm, later_recv[0, :, half:, :])
    record(1, half, late_norm, later_recv[1, :, half:, :])
    for k in range(2):
        wait(first_recv.at[k], first_out.at[k])
        wait(later_recv.at[k], later_out.at[k])
    pltpu.make_async_copy(examples.at[peers], examples.at[peers], emb_out).wait()

    @pl.loop(0, pieces)
    def _(c):
        sent = pl.ds(0, n - 1)
        pltpu.make_async_copy(outgoing.at[c, sent], outgoing.at[c, sent], out_sem.at[c]).wait()


def update_kernel(
    rate, early_ref, turned_ref, total_ref, losses_in, out_ref, losses_ref, held, out_sem
):
    chunks, model_width, width = held.shape
    losses_ref[...] = losses_in[...]
    copies = []
    for c in range(chunks):
        for i in range(model_width // ROW_TILE):
            here = pl.ds(i * ROW_TILE, ROW_TILE)
            held[c, here, :] = early_ref[c, here, :] - rate * jnp.dot(
                turned_ref[here, :], total_ref[c], preferred_element_type=jnp.float32
            )
            copies.append(
                pltpu.make_async_copy(
                    held.at[c, here],
                    out_ref.at[here, pl.ds(c * width, width)],
                    out_sem.at[c, i],
                )
            )
            copies[-1].start()
    for copy in copies:
        copy.wait()


def fused(embeddings, weights, labels):
    cls_n, row_n = lax.axis_size("cls"), lax.axis_size("row")
    n = cls_n * row_n
    shard_rows, model_width = embeddings.shape
    rows = shard_rows * row_n
    features = weights.shape[0]
    class_count = weights.shape[1] // n
    width = max(w for w in (128, 256, 384, 512) if class_count % w == 0)
    narrow = 256 if width % 256 == 0 else LANES
    chunks = class_count // width
    pieces = class_count // narrow
    rate = learn_rate / rows
    slabs = rows // LANES
    half_rows = rows // 2
    vmem = pl.BlockSpec(memory_space=pltpu.VMEM)
    hbm = pl.BlockSpec(memory_space=pltpu.HBM)
    dma = pltpu.SemaphoreType.DMA
    lanes = pltpu.VMEM((rows, LANES), jnp.float32)
    operands = (embeddings, weights, labels.reshape(slabs, LANES))
    early, late, turned, losses = pl.pallas_call(
        functools.partial(exchange_kernel, cls_n, row_n, rate),
        out_shape=(
            jax.ShapeDtypeStruct((chunks, model_width, width), jnp.float32),
            jax.ShapeDtypeStruct((chunks, half_rows, width), jnp.bfloat16),
            jax.ShapeDtypeStruct((model_width, half_rows), jnp.bfloat16),
            jax.ShapeDtypeStruct((STEPS, rows), jnp.float32),
        ),
        in_specs=[hbm, hbm, hbm],
        out_specs=(vmem, vmem, vmem, vmem),
        scratch_shapes=[
            pltpu.VMEM((2, n, features, narrow), jnp.float32),
            pltpu.VMEM((pieces, n, features, narrow), jnp.bfloat16),
            pltpu.VMEM((chunks, n * features, width), jnp.bfloat16),
            pltpu.VMEM((rows, LANES), jnp.int32),
            pltpu.VMEM((chunks, rows, width), jnp.float32),
            pltpu.VMEM((rows, rows), jnp.bfloat16),
            pltpu.VMEM((rows, model_width), jnp.bfloat16),
            pltpu.VMEM((model_width, half_rows), jnp.bfloat16),
            pltpu.VMEM((shard_rows, model_width), jnp.float32),
            pltpu.VMEM((shard_rows, model_width), jnp.bfloat16),
            pltpu.VMEM((slabs, LANES), jnp.int32),
            lanes,
            lanes,
            lanes,
            lanes,
            lanes,
            pltpu.VMEM((2, slabs, LANES), jnp.float32),
            pltpu.VMEM((2, n, slabs, LANES), jnp.float32),
            pltpu.VMEM((2, slabs, LANES), jnp.float32),
            pltpu.VMEM((2, n, slabs, LANES), jnp.float32),
            dma((2,)),
            dma((2,)),
            dma((pieces,)),
            dma((pieces,)),
            dma,
            dma,
            dma((2,)),
            dma((2,)),
            dma((2,)),
            dma((2,)),
        ],
        compiler_params=pltpu.CompilerParams(
            collective_id=0, has_side_effects=True, vmem_limit_bytes=KERNEL_VMEM
        ),
    )(*(pltpu.with_memory_space_constraint(x, pltpu.HBM) for x in operands))
    update, losses = pl.pallas_call(
        functools.partial(update_kernel, rate),
        out_shape=(
            jax.ShapeDtypeStruct((model_width, class_count), jnp.float32),
            jax.ShapeDtypeStruct((STEPS, rows), jnp.float32),
        ),
        in_specs=[vmem, vmem, vmem, vmem],
        out_specs=(hbm, vmem),
        scratch_shapes=[
            pltpu.VMEM((chunks, model_width, width), jnp.float32),
            dma((chunks, model_width // ROW_TILE)),
        ],
        compiler_params=pltpu.CompilerParams(vmem_limit_bytes=UPDATE_VMEM),
    )(early, turned, late, losses)
    return update, losses


def shards(embeddings, weights, labels):
    rows = embeddings.shape[0] * lax.axis_size("row")
    square = rows == embeddings.shape[1]
    if STEPS == 2 and square and weights.shape[0] % 16 == 0:
        return fused(embeddings, weights, labels)
    peer_count = lax.axis_size(("cls", "row"))
    examples = lax.all_gather(embeddings.astype(jnp.bfloat16), "row", axis=0, tiled=True)
    row_count = examples.shape[0]
    feature_rows = weights.shape[0]
    class_count = weights.shape[1] // peer_count
    offset = lax.axis_index(("cls", "row")) * class_count
    columns = lax.broadcasted_iota(jnp.int32, (1, class_count), 1) + offset
    label_hit = columns == labels[:, None]
    pieces = weights.astype(jnp.bfloat16).reshape(feature_rows, peer_count, class_count)
    block_weights = lax.all_to_all(
        pieces.transpose(1, 0, 2), ("cls", "row"), split_axis=0, concat_axis=0, tiled=True
    )
    flat_weights = block_weights.reshape(peer_count * feature_rows, class_count)
    first_logits = jnp.dot(examples, flat_weights, preferred_element_type=jnp.float32)
    rate = learn_rate / row_count
    gram = lax.dot_general(
        examples, examples, (((1,), (1,)), ((), ())), preferred_element_type=jnp.float32
    ).astype(jnp.bfloat16)
    total = None
    loss_rows = []
    for step_index in range(STEPS):
        logits = first_logits
        if step_index > 0:
            logits = logits - rate * jnp.dot(gram, total, preferred_element_type=jnp.float32)
        local_peak = jnp.max(logits, axis=1)
        local_total = jnp.sum(jnp.exp(logits - local_peak[:, None]), axis=1)
        local_picked = jnp.sum(jnp.where(label_hit, logits, 0.0), axis=1)
        stats = lax.all_gather(
            jnp.stack([local_peak, local_total, local_picked]), ("cls", "row"), axis=0
        )
        row_peak = jnp.max(stats[:, 0], axis=0)
        row_total = jnp.sum(stats[:, 1] * jnp.exp(stats[:, 0] - row_peak[None, :]), axis=0)
        picked = jnp.sum(stats[:, 2], axis=0)
        log_norm = row_peak + jnp.log(row_total)
        loss_rows.append(log_norm - picked)
        onehot = jnp.where(label_hit, 1.0, 0.0)
        residual = jnp.exp(logits - log_norm[:, None]) - onehot
        if total is not None:
            residual = residual + total.astype(jnp.float32)
        total = residual.astype(jnp.bfloat16)
    update = lax.dot_general(
        examples, total, (((0,), (0,)), ((), ())), preferred_element_type=jnp.float32
    )
    return (-rate * update, jnp.stack(loss_rows))


def solution(mesh):
    placed = (P("row", None), P(("cls", "row"), None), P())
    return jax.shard_map(
        shards,
        mesh=mesh,
        in_specs=placed,
        out_specs=(P(None, ("cls", "row")), P()),
        check_vma=False,
    )
```
